32 devices in a mesh: dom: 8 (over z, x), sub: 4 (over y, core).
Axes of the slice: x: 2, y: 2, z: 4, core: 2. Of those that a mesh axis runs over, the one named last changes fastest.
Arguments:
- features: bfloat16 [32768, 256], P(('dom', 'sub')), may hold values from -16 to 16
- weight: bfloat16 [256, 256], replicated, may hold values from -0.375 to 0.375
- send_far: int32 [16384], P(('dom', 'sub')), may hold values from 0 to 1023
- send_near: int32 [4096], P(('dom', 'sub')), may hold values from 0 to 1023
- tile_dst: int32 [512], P(('dom', 'sub')), may hold values from 0 to 7
- inner_src: int32 [256], P(('dom', 'sub')), may hold values from 0 to 7
- outer_src: int32 [256], P(('dom', 'sub')), may hold values from 0 to 4
- tile_live: int32 [32, 2], P(('dom', 'sub')), may hold values from 4 to 8
- tile_weight: bfloat16 [512, 128, 128], P(('dom', 'sub')), may hold values from -0.3125 to 0.3125
Outputs:
- whitened: bfloat16 [32768, 256], P(('dom', 'sub'))
- loss_value: float32 [], replicated
The draws below stay inside these ranges and needn't reach their ends.
Inputs may be any that keep to these rules, and one draw needn't show every extreme that they name: `send_far`: rows may repeat. `tile_live`: live slots come first in each half of a device's slots.
All inputs are finite; a program needn't handle non-finite values.
Results may differ from the reference program's by a relative error of at most 0.0085.
Values may be sent and summed in bfloat16 or wider, within the bound.
A program may use at most 64 MiB of HBM per device.

```python
import jax
import jax.numpy as jnp
from jax import lax

F = 256
B = 128
V_DEV = 1024
HALO_DOM = 512
SLOTS = 8
HALO_SUB = 128
PEER_DOM = 64
PEER_SUB = 32
VERTS = 32768
N_DOM = 8
N_SUB = 4


def draw_features(key, part):
    key_base = jax.random.fold_in(key, 11)
    key_jitter = jax.random.fold_in(key, 14)
    key_shift = jax.random.fold_in(key, 15)
    key_heavy = jax.random.fold_in(key, 16)
    key_sign = jax.random.fold_in(key, 17)
    block_count = VERTS // V_DEV
    block_index = jnp.arange(block_count, dtype=jnp.int32)
    sub_place = (block_index % N_SUB).astype(jnp.float32) / max(N_SUB - 1, 1)
    dom_place = (block_index // N_SUB).astype(jnp.float32) / max(block_count // N_SUB - 1, 1)
    jitter = jax.random.uniform(key_jitter, (block_count,), jnp.float32, -0.3, 0.3)
    block_scale = jnp.exp(-0.6 + 0.6 * sub_place + 0.5 * dom_place + jitter)
    block_shift = jax.random.uniform(key_shift, (block_count, 1, F), jnp.float32, -0.5, 0.5)
    array_shape = (block_count, V_DEV, F)
    base_values = jnp.clip(jax.random.normal(key_base, array_shape, jnp.float32), -6.0, 6.0)
    values = base_values * block_scale[:, None, None] + block_shift
    values = jnp.clip(values, -9.0, 9.0)
    heavy_noise = jnp.clip(jax.random.normal(key_heavy, (block_count, V_DEV, 1), jnp.float32), -2.5, 2.5)
    block_sign = jnp.where(jax.random.bernoulli(key_sign, 0.5, (block_count, 1, 1)), 1.0, -1.0).astype(jnp.float32)
    heavy_values = block_sign * (12.0 + 1.5 * heavy_noise)
    column_index = jnp.arange(F, dtype=jnp.int32)
    heavy_mask = column_index[None, None, :] == (block_index % F)[:, None, None]
    values = jnp.where(heavy_mask, heavy_values, values)
    values = jnp.clip(values, -16.0, 16.0).reshape(VERTS, F)
    return values.astype(jnp.bfloat16)


def plant(entries, own_key, least, top_value):
    longest = entries.shape.index(max(entries.shape))
    spots = []
    for shift in (0, 1):
        where = [jax.random.randint(jax.random.fold_in(own_key, axis), (), 0, length) for axis, length in enumerate(entries.shape)]
        where[longest] = (where[longest] + shift) % entries.shape[longest]
        spots.append(tuple(where))
    return entries.at[spots[0]].set(least).at[spots[1]].set(top_value)


def steps_of(stream_key, shape, cuts, low, top_value):
    def one(dim, parts):
        heights = jax.random.uniform(jax.random.fold_in(jax.random.fold_in(stream_key, 6), dim), (parts,), jnp.float32, low / len(cuts), top_value / len(cuts))
        return jnp.repeat(jnp.exp(heights), shape[dim] // parts).reshape((-1,) + (1,) * (len(shape) - dim - 1))

    loudness = one(*cuts[0])
    for cut in cuts[1:]:
        loudness = loudness * one(*cut)
    return loudness


def normal_values(key, extent, deviation, limit, pieces=(), kind=jnp.bfloat16):
    level = steps_of(key, extent, pieces, -0.22, 0.18) if pieces else 1.0
    result = jax.random.normal(key, extent, jnp.float32) * deviation * level
    return jnp.minimum(jnp.maximum(result, -limit), limit).astype(kind)


def setup_inputs(seed: int = 0) -> dict:
    key_of = jax.random.split(jax.random.key(seed), 10)
    return {
        "features": draw_features(jax.random.fold_in(key_of[9], 71), 0),
        "weight": normal_values(key_of[1], (F, F), F ** -0.5, 0.375),
        "send_far": plant(jax.random.randint(key_of[2], (N_DOM * N_SUB * HALO_DOM,), 0, V_DEV), jax.random.fold_in(key_of[2], 1), 0, V_DEV - 1).astype(jnp.int32),
        "send_near": plant(jax.random.randint(key_of[3], (N_DOM * N_SUB * HALO_SUB,), 0, V_DEV), jax.random.fold_in(key_of[3], 1), 0, V_DEV - 1).astype(jnp.int32),
        "tile_dst": plant(jax.random.randint(key_of[4], (N_DOM * N_SUB * 2 * SLOTS,), 0, V_DEV // B), jax.random.fold_in(key_of[4], 1), 0, (V_DEV // B) - 1).astype(jnp.int32),
        "inner_src": plant(jax.random.randint(key_of[5], (N_DOM * N_SUB * SLOTS,), 0, V_DEV // B), jax.random.fold_in(key_of[5], 1), 0, (V_DEV // B) - 1).astype(jnp.int32),
        "outer_src": plant(jax.random.randint(key_of[6], (N_DOM * N_SUB * SLOTS,), 0, (HALO_DOM + HALO_SUB) // B), jax.random.fold_in(key_of[6], 1), 0, ((HALO_DOM + HALO_SUB) // B) - 1).astype(jnp.int32),
        "tile_live": plant(jax.random.randint(key_of[7], (N_DOM * N_SUB, 2), SLOTS // 2, SLOTS + 1), jax.random.fold_in(key_of[7], 1), SLOTS // 2, SLOTS).astype(jnp.int32),
        "tile_weight": normal_values(key_of[8], (N_DOM * N_SUB * 2 * SLOTS, B, B), (3 * B) ** -0.5, 0.3125, ((0, 32),)),
    }


epsilon = 1e-05

def whiten_map(gram_sum, vertex_count, feat_width):
    identity = jnp.eye(feat_width, dtype=jnp.float32)
    scaled = gram_sum / vertex_count + epsilon * identity
    lower = jnp.linalg.cholesky(scaled)
    inverse = lax.linalg.triangular_solve(lower, identity, left_side=True, lower=True)
    return inverse.T

def reference(features, weight, send_far, send_near, tile_dst, inner_src, outer_src, tile_live, tile_weight):
    device_total = N_DOM * N_SUB
    local_tiles = V_DEV // B
    blocks = features.reshape(N_DOM, N_SUB, V_DEV, F)
    far_lists = send_far.reshape(N_DOM, N_SUB, N_DOM, PEER_DOM)
    near_lists = send_near.reshape(N_DOM, N_SUB, N_SUB, PEER_SUB)
    dest_tiles = tile_dst.reshape(device_total, 2 * SLOTS)
    inner_tiles = inner_src.reshape(device_total, SLOTS)
    outer_tiles = outer_src.reshape(device_total, SLOTS)
    slot_weights = tile_weight.reshape(device_total, 2 * SLOTS, B, B)

    def per_device(device_index):
        dom_index = device_index // N_SUB
        sub_index = device_index % N_SUB
        same_sub = blocks[:, sub_index]
        far_index = far_lists[:, sub_index, dom_index, :]
        far_rows = jnp.take_along_axis(same_sub, far_index[:, :, None], axis=1).reshape(HALO_DOM, F)
        same_dom = blocks[dom_index]
        near_index = near_lists[dom_index, :, sub_index, :]
        near_rows = jnp.take_along_axis(same_dom, near_index[:, :, None], axis=1).reshape(HALO_SUB, F)
        own_rows = blocks[dom_index, sub_index]
        tile_table = jnp.concatenate([own_rows, far_rows, near_rows], 0).reshape(-1, B, F).astype(jnp.float32)
        source_tiles = jnp.concatenate([inner_tiles[device_index], outer_tiles[device_index] + local_tiles])
        selected = tile_table[source_tiles]
        products = jnp.einsum('kij,kjf->kif', slot_weights[device_index].astype(jnp.float32), selected, precision=lax.Precision.HIGHEST)
        slot_index = jnp.arange(SLOTS, dtype=jnp.int32)
        slot_mask = jnp.concatenate([slot_index < tile_live[device_index, 0], slot_index < tile_live[device_index, 1]])
        tile_index = jnp.arange(local_tiles, dtype=jnp.int32)
        selector = ((dest_tiles[device_index][None, :] == tile_index[:, None]) & slot_mask[None, :]).astype(jnp.float32)
        summed = jnp.einsum('tk,kif->tif', selector, products, precision=lax.Precision.HIGHEST).reshape(V_DEV, F)
        aggregate = summed.astype(jnp.bfloat16)
        projected = jnp.dot(aggregate.astype(jnp.float32), weight.astype(jnp.float32), preferred_element_type=jnp.float32)
        return (own_rows.astype(jnp.float32) + jax.nn.silu(projected)).astype(jnp.bfloat16)
    hidden = lax.map(per_device, jnp.arange(device_total, dtype=jnp.int32)).reshape(VERTS, F)
    gram_sum = lax.dot_general(hidden.astype(jnp.float32), hidden.astype(jnp.float32), (((0,), (0,)), ((), ())), preferred_element_type=jnp.float32)
    whitener = whiten_map(gram_sum, VERTS, F)
    white = jnp.dot(hidden.astype(jnp.float32), whitener, precision=lax.Precision.HIGHEST)
    distance = white - features.astype(jnp.float32)
    loss_value = jnp.sum(distance * distance) / (VERTS * F)
    return (white.astype(jnp.bfloat16), loss_value)
```

```python
import functools

import jax
import jax.numpy as jnp
from jax import lax
from jax.experimental import pallas as pl
from jax.experimental.pallas import tpu as pltpu
from jax.sharding import PartitionSpec as P

epsilon = 1e-05
MESH = pl.DeviceIdType.MESH
LEAF = 64
HIGH = lax.Precision.HIGHEST


def one_hot_rows(index_row, row_count):
    rows = index_row.shape[1]
    columns = jnp.broadcast_to(index_row, (128, rows)).T
    lane = lax.broadcasted_iota(jnp.int32, (rows, 128), 1)
    parts = [
        jnp.where(columns == lane + start, 1.0, 0.0).astype(jnp.bfloat16)
        for start in range(0, row_count, 128)
    ]
    return jnp.concatenate(parts, axis=1)


def padded_rows(count):
    return -(-count // 16) * 16


def packing(packed_rows, padded_total, n_dom, n_sub, per_dom, per_sub, near_rows_each):
    near_total = n_sub * near_rows_each
    far_total = packed_rows - near_total
    far_rows_each = far_total // n_dom
    row = lax.broadcasted_iota(jnp.int32, (packed_rows, padded_total), 0)
    column = lax.broadcasted_iota(jnp.int32, (packed_rows, padded_total), 1)
    far_place = row + lax.div(row, far_rows_each) * (per_dom - far_rows_each)
    near_row = row - far_total
    near_place = (
        n_dom * per_dom + near_row + lax.div(near_row, near_rows_each) * (per_sub - near_rows_each)
    )
    place = jnp.where(row < far_total, far_place, near_place)
    return jnp.where(place == column, 1.0, 0.0).astype(jnp.bfloat16)


def leaf_inverse(block):
    size = block.shape[0]
    row = lax.broadcasted_iota(jnp.int32, (size, size), 0)
    lane = lax.broadcasted_iota(jnp.int32, (size, size), 1)
    work = jnp.concatenate([block, jnp.where(row == lane, 1.0, 0.0)], axis=1)
    wide_row = lax.broadcasted_iota(jnp.int32, (size, 1), 0)
    for step in range(size - 1):
        pivot_row = work[step : step + 1, :]
        scaled = pivot_row * (1.0 / pivot_row[:, step : step + 1])
        column = work[:, step : step + 1]
        work = work - jnp.where(wide_row > step, column, 0.0) * scaled
    diagonal = jnp.sum(jnp.where(row == lane, work[:, :size], 0.0), axis=1, keepdims=True)
    return work[:, size:] * (1.0 / jnp.sqrt(diagonal))


def kernel(
    n_dom,
    n_sub,
    near_each,
    features_ref,
    weight_ref,
    far_ref,
    near_ref,
    dst_ref,
    inner_ref,
    outer_ref,
    live_ref,
    tile_ref,
    out_ref,
    loss_ref,
    far_send,
    near_send,
    arrived,
    table,
    products,
    acc,
    aggregate,
    gram_part,
    cross_part,
    gram_in,
    cross_in,
    gram_own,
    cross_own,
    gram,
    cross,
    work,
    halo_sems,
    sum_sems,
):
    total_devices = n_dom * n_sub
    dom = lax.axis_index("dom")
    sub = lax.axis_index("sub")
    me = dom * n_sub + sub
    tiles, size, feat = features_ref.shape
    rows = tiles * size
    slots = inner_ref.shape[0]
    owners = min(total_devices, feat // 8)
    share = feat // owners
    own_rows = pl.ds(pl.multiple_of(lax.rem(me, owners) * share, share), share)

    def device_of(index):
        return (lax.div(index, n_sub), lax.rem(index, n_sub))

    barrier = pltpu.get_barrier_semaphore()

    @pl.loop(1, total_devices)
    def _(offset):
        peer = lax.rem(me + offset, total_devices)
        pl.semaphore_signal(barrier, inc=1, device_id=device_of(peer), device_id_type=MESH)

    features = features_ref[...].reshape(rows, feat)
    far_rows = jnp.dot(
        one_hot_rows(far_ref[...], rows), features, preferred_element_type=jnp.float32
    ).astype(jnp.bfloat16)
    near_rows = jnp.dot(
        one_hot_rows(near_ref[...], rows), features, preferred_element_type=jnp.float32
    ).astype(jnp.bfloat16)
    far_send[...] = far_rows
    near_send[...] = near_rows
    per_dom = far_send.shape[0] // n_dom
    per_sub = near_send.shape[0] // n_sub
    far_count = per_dom * n_dom
    packed = size % per_dom == 0 and size % per_sub == 0 and arrived.shape[0] == table.shape[0] * size

    def place(first, count):
        if packed:
            within = pl.multiple_of(lax.rem(first, size), count)
            return table.at[lax.div(first, size), pl.ds(within, count)]
        return arrived.at[pl.ds(pl.multiple_of(first, count), count)]

    def dom_rows(index):
        return pl.ds(pl.multiple_of(index * per_dom, per_dom), per_dom)

    def sub_rows(index):
        return pl.ds(pl.multiple_of(index * per_sub, per_sub), per_sub)

    def dom_place(index):
        return place(index * per_dom, per_dom)

    def sub_place(index):
        return place(far_count + index * per_sub, per_sub)

    pl.semaphore_wait(barrier, total_devices - 1)

    @pl.loop(1, n_dom)
    def _(offset):
        peer = lax.rem(dom + offset, n_dom)
        pltpu.make_async_remote_copy(
            src_ref=far_send.at[dom_rows(peer)],
            dst_ref=dom_place(dom),
            send_sem=halo_sems.at[0],
            recv_sem=halo_sems.at[1],
            device_id=(peer, sub),
            device_id_type=MESH,
        ).start()

    @pl.loop(1, n_sub)
    def _(offset):
        peer = lax.rem(sub + offset, n_sub)
        pltpu.make_async_remote_copy(
            src_ref=near_send.at[sub_rows(peer)],
            dst_ref=sub_place(sub),
            send_sem=halo_sems.at[2],
            recv_sem=halo_sems.at[3],
            device_id=(dom, peer),
            device_id_type=MESH,
        ).start()

    dom_place(dom)[...] = far_send[dom_rows(dom), :]
    sub_place(sub)[...] = near_send[sub_rows(sub), :]

    def slot_products(rows_ref, source, first):
        for slot in range(slots):
            products[slot] = jnp.dot(
                tile_ref[first + slot],
                rows_ref[source[slot]],
                preferred_element_type=jnp.float32,
            )

    def slot_sum(tile, first, count):
        total = None
        for slot in range(slots):
            target = jnp.full((1, feat), dst_ref[first + slot], jnp.int32)
            chosen = jnp.where(jnp.logical_and(target == tile, count > slot), 1.0, 0.0)
            term = products[slot] * chosen
            total = term if total is None else total + term
        return total

    slot_products(features_ref, inner_ref, 0)
    inner_count = jnp.full((1, feat), live_ref[0, 0], jnp.int32)
    outer_count = jnp.full((1, feat), live_ref[0, 1], jnp.int32)

    @pl.loop(0, tiles)
    def _(tile):
        acc[tile] = slot_sum(tile, 0, inner_count)

    features_t = features.T
    wide = features.astype(jnp.float32)
    square = jnp.sum(wide * wide)
    cross_part[:, feat:] = jnp.broadcast_to(square, (feat, cross_part.shape[1] - feat))

    def settle(ref, sem):
        pltpu.make_async_copy(ref, ref, sem).wait()

    settle(arrived.at[pl.ds(0, per_dom * (n_dom - 1))], halo_sems.at[1])
    settle(arrived.at[pl.ds(0, per_sub * (n_sub - 1))], halo_sems.at[3])
    if not packed:
        table[...] = jnp.dot(
            packing(table.shape[0] * size, arrived.shape[0], n_dom, n_sub, per_dom, per_sub, near_each),
            arrived[...],
            preferred_element_type=jnp.float32,
        ).astype(jnp.bfloat16).reshape(table.shape)
    slot_products(table, outer_ref, slots)

    @pl.loop(0, tiles)
    def _(tile):
        total = acc[tile] + slot_sum(tile, slots, outer_count)
        aggregate[pl.ds(pl.multiple_of(tile * size, size), size), :] = total.astype(jnp.bfloat16)

    projected = jnp.dot(aggregate[...], weight_ref[...], preferred_element_type=jnp.float32)
    hidden = (
        features_ref[...].reshape(rows, feat).astype(jnp.float32) + projected / (1.0 + jnp.exp(-projected))
    ).astype(jnp.bfloat16)
    gram_part[...] = jnp.dot(hidden.T, hidden, preferred_element_type=jnp.float32)

    def scatter(part, landing, first):
        def send(offset):
            peer = lax.rem(me + offset, total_devices)

            def go():
                pltpu.make_async_remote_copy(
                    src_ref=part.at[pl.ds(pl.multiple_of(peer * share, share), share)],
                    dst_ref=landing.at[me],
                    send_sem=sum_sems.at[first],
                    recv_sem=sum_sems.at[first + 1],
                    device_id=device_of(peer),
                    device_id_type=MESH,
                ).start()

            if owners == total_devices:
                go()
            else:
                pl.when(peer < owners)(go)

        pl.loop(1, total_devices)(send)

    def reduce_and_gather(part, landing, own, full, first):
        def go():
            landing[me] = part[own_rows, :]
            settle(landing.at[pl.ds(0, total_devices - 1)], sum_sems.at[first + 1])
            total = jnp.sum(landing[...], axis=0)
            own[...] = total
            full[own_rows, :] = total

            @pl.loop(1, total_devices)
            def _(offset):
                peer = lax.rem(me + offset, total_devices)
                pltpu.make_async_remote_copy(
                    src_ref=own,
                    dst_ref=full.at[own_rows],
                    send_sem=sum_sems.at[first + 2],
                    recv_sem=sum_sems.at[first + 3],
                    device_id=device_of(peer),
                    device_id_type=MESH,
                ).start()

        if owners == total_devices:
            go()
        else:
            pl.when(me < owners)(go)

    def finish(part, landing, full, first):
        def owner():
            settle(full.at[pl.ds(0, share * (owners - 1))], sum_sems.at[first + 3])

        def other():
            settle(full, sum_sems.at[first + 3])

        if owners == total_devices:
            owner()
        else:
            pl.when(me < owners)(owner)
            pl.when(me >= owners)(other)

    def drain(part, landing, first):
        def owner():
            settle(part.at[pl.ds(0, share * (owners - 1))], sum_sems.at[first])
            settle(landing.at[pl.ds(0, total_devices - 1)], sum_sems.at[first + 2])

        def other():
            settle(part, sum_sems.at[first])

        if owners == total_devices:
            owner()
        else:
            pl.when(me < owners)(owner)
            pl.when(me >= owners)(other)

    scatter(gram_part, gram_in, 0)
    cross_part[:, :feat] = jnp.dot(features_t, hidden, preferred_element_type=jnp.float32)
    reduce_and_gather(gram_part, gram_in, gram_own, gram, 0)
    scatter(cross_part, cross_in, 4)
    finish(gram_part, gram_in, gram, 0)

    vertex_count = rows * total_devices
    diagonal = lax.broadcasted_iota(jnp.int32, (feat, feat), 0) == lax.broadcasted_iota(
        jnp.int32, (feat, feat), 1
    )
    identity = jnp.where(diagonal, 1.0, 0.0)
    work[:, :feat] = gram[...] / vertex_count + epsilon * identity
    work[:, feat:] = identity
    for start in range(0, feat, LEAF):
        stop = start + LEAF
        inverse = leaf_inverse(work[start:stop, start:stop])
        pivot_rows = jnp.dot(
            inverse, work[start:stop, :], precision=HIGH, preferred_element_type=jnp.float32
        )
        work[start:stop, :] = pivot_rows
        if stop < feat:
            work[stop:, :] = work[stop:, :] - lax.dot_general(
                pivot_rows[:, stop:feat],
                pivot_rows,
                (((0,), (0,)), ((), ())),
                precision=HIGH,
                preferred_element_type=jnp.float32,
            )
        if start == LEAF:
            reduce_and_gather(cross_part, cross_in, cross_own, cross, 4)

    lower_inverse = work[:, feat:]
    high_part = lower_inverse.astype(jnp.bfloat16)
    low_part = (lower_inverse - high_part.astype(jnp.float32)).astype(jnp.bfloat16)
    across = (((1,), (1,)), ((), ()))
    white = lax.dot_general(
        hidden, high_part, across, preferred_element_type=jnp.float32
    ) + lax.dot_general(hidden, low_part, across, preferred_element_type=jnp.float32)
    out_ref[...] = white.astype(jnp.bfloat16)

    whitened_gram = jnp.dot(
        lower_inverse, gram[...], precision=HIGH, preferred_element_type=jnp.float32
    )
    finish(cross_part, cross_in, cross, 4)
    distance = jnp.sum(lower_inverse * (whitened_gram - 2.0 * cross[:, :feat]))
    square_sum = jnp.max(cross[0:8, feat:])
    loss_ref[0, 0] = (distance + square_sum) / (vertex_count * feat)

    settle(far_send.at[pl.ds(0, per_dom * (n_dom - 1))], halo_sems.at[0])
    settle(near_send.at[pl.ds(0, per_sub * (n_sub - 1))], halo_sems.at[2])
    drain(gram_part, gram_in, 0)
    drain(cross_part, cross_in, 4)


def body(
    n_dom,
    n_sub,
    features,
    weight,
    send_far,
    send_near,
    tile_dst,
    inner_src,
    outer_src,
    tile_live,
    tile_weight,
):
    rows, feat = features.shape
    size = tile_weight.shape[1]
    slots = inner_src.shape[0]
    total = n_dom * n_sub
    share = feat // min(total, feat // 8)
    far_count = send_far.shape[0]
    near_count = send_near.shape[0]

    def padded(index, peers):
        each = index.shape[0] // peers
        grid = index.reshape(peers, each)
        return jnp.pad(grid, ((0, 0), (0, padded_rows(each) - each))).reshape(1, -1)

    far_index = padded(send_far, n_dom)
    near_index = padded(send_near, n_sub)
    far_padded = far_index.shape[1]
    near_padded = near_index.shape[1]
    vmem = pl.BlockSpec(memory_space=pltpu.VMEM)
    smem = pl.BlockSpec(memory_space=pltpu.SMEM)
    f32 = jnp.float32
    bf16 = jnp.bfloat16
    cross_width = feat + 128
    whitened, loss = pl.pallas_call(
        functools.partial(kernel, n_dom, n_sub, near_count // n_sub),
        out_shape=(
            jax.ShapeDtypeStruct((rows, feat), bf16),
            jax.ShapeDtypeStruct((1, 1), f32),
        ),
        in_specs=[vmem, vmem, vmem, vmem, smem, smem, smem, smem, vmem],
        out_specs=(vmem, smem),
        scratch_shapes=[
            pltpu.VMEM((far_padded, feat), bf16),
            pltpu.VMEM((near_padded, feat), bf16),
            pltpu.VMEM((far_padded + near_padded, feat), bf16),
            pltpu.VMEM(((far_count + near_count) // size, size, feat), bf16),
            pltpu.VMEM((slots, size, feat), f32),
            pltpu.VMEM((rows // size, size, feat), f32),
            pltpu.VMEM((rows, feat), bf16),
            pltpu.VMEM((feat, feat), f32),
            pltpu.VMEM((feat, cross_width), f32),
            pltpu.VMEM((total, share, feat), f32),
            pltpu.VMEM((total, share, cross_width), f32),
            pltpu.VMEM((share, feat), f32),
            pltpu.VMEM((share, cross_width), f32),
            pltpu.VMEM((feat, feat), f32),
            pltpu.VMEM((feat, cross_width), f32),
            pltpu.VMEM((feat, 2 * feat), f32),
            pltpu.SemaphoreType.DMA((4,)),
            pltpu.SemaphoreType.DMA((8,)),
        ],
        compiler_params=pltpu.CompilerParams(collective_id=0, has_side_effects=True),
    )(
        features.reshape(rows // size, size, feat),
        weight,
        far_index,
        near_index,
        tile_dst,
        inner_src,
        outer_src,
        tile_live,
        tile_weight,
    )
    return whitened, loss.reshape(())


def solution(mesh):
    placed = (
        P(("dom", "sub"), None),
        P(),
        P(("dom", "sub")),
        P(("dom", "sub")),
        P(("dom", "sub")),
        P(("dom", "sub")),
        P(("dom", "sub")),
        P(("dom", "sub"), None),
        P(("dom", "sub"), None, None),
    )
    return jax.shard_map(
        functools.partial(body, mesh.shape["dom"], mesh.shape["sub"]),
        mesh=mesh,
        in_specs=placed,
        out_specs=(P(("dom", "sub"), None), P()),
        check_vma=False,
    )
```

```python
import functools

import jax
import jax.numpy as jnp
from jax import lax
from jax.experimental import pallas as pl
from jax.experimental.pallas import tpu as pltpu
from jax.sharding import PartitionSpec as P

epsilon = 1e-05
MESH = pl.DeviceIdType.MESH
LEAF = 64
HIGH = lax.Precision.HIGHEST


def one_hot_rows(index_row, row_count):
    rows = index_row.shape[1]
    columns = jnp.broadcast_to(index_row, (128, rows)).T
    lane = lax.broadcasted_iota(jnp.int32, (rows, 128), 1)
    parts = [
        jnp.where(columns == lane + start, 1.0, 0.0).astype(jnp.bfloat16)
        for start in range(0, row_count, 128)
    ]
    return jnp.concatenate(parts, axis=1)


def padded_rows(count):
    return -(-count // 16) * 16


def packing(packed_rows, padded_total, n_dom, n_sub, per_dom, per_sub, near_rows_each):
    near_total = n_sub * near_rows_each
    far_total = packed_rows - near_total
    far_rows_each = far_total // n_dom
    row = lax.broadcasted_iota(jnp.int32, (packed_rows, padded_total), 0)
    column = lax.broadcasted_iota(jnp.int32, (packed_rows, padded_total), 1)
    far_place = row + lax.div(row, far_rows_each) * (per_dom - far_rows_each)
    near_row = row - far_total
    near_place = (
        n_dom * per_dom + near_row + lax.div(near_row, near_rows_each) * (per_sub - near_rows_each)
    )
    place = jnp.where(row < far_total, far_place, near_place)
    return jnp.where(place == column, 1.0, 0.0).astype(jnp.bfloat16)


def leaf_inverse(block):
    size = block.shape[0]
    row = lax.broadcasted_iota(jnp.int32, (size, size), 0)
    lane = lax.broadcasted_iota(jnp.int32, (size, size), 1)
    work = jnp.concatenate([block, jnp.where(row == lane, 1.0, 0.0)], axis=1)
    tall = lax.broadcasted_iota(jnp.int32, (size, 1), 0)
    for step in range(0, size - 2, 2):
        first = work[step : step + 1, :]
        second = work[step + 1 : step + 2, :]
        a = first[:, step : step + 1]
        b = first[:, step + 1 : step + 2]
        c = second[:, step + 1 : step + 2]
        scale = 1.0 / (a * c - b * b)
        upper = (c * first - b * second) * scale
        lower = (a * second - b * first) * scale
        below = tall > step + 1
        work = (
            work
            - jnp.where(below, work[:, step : step + 1], 0.0) * upper
            - jnp.where(below, work[:, step + 1 : step + 2], 0.0) * lower
        )
    left = work[:, :size]
    diagonal = jnp.sum(jnp.where(row == lane, left, 0.0), axis=1, keepdims=True)
    before = jnp.sum(jnp.where(row == lane + 1, left, 0.0), axis=1, keepdims=True)
    odd = lax.rem(tall, 2) == 1
    above = pltpu.roll(jnp.broadcast_to(diagonal, (size, 2 * size)), 1, 0)
    factor = jnp.where(odd, before, 0.0) / above
    work = work - factor * pltpu.roll(work, 1, 0)
    diagonal = jnp.sum(jnp.where(row == lane, work[:, :size], 0.0), axis=1, keepdims=True)
    return work[:, size:] * (1.0 / jnp.sqrt(diagonal))


def kernel(
    n_dom,
    n_sub,
    near_each,
    features_in,
    weight_in,
    far_in,
    near_in,
    dst_in,
    inner_in,
    outer_in,
    live_in,
    tile_in,
    out_ref,
    loss_ref,
    features_ref,
    weight_ref,
    far_ref,
    near_ref,
    dst_ref,
    inner_ref,
    outer_ref,
    live_ref,
    tile_ref,
    result,
    far_send,
    near_send,
    arrived,
    table,
    products,
    acc,
    aggregate,
    gram_part,
    gram_in,
    gram_own,
    gram,
    loss_own,
    loss_all,
    work,
    load_sems,
    halo_sems,
    sum_sems,
):
    total_devices = n_dom * n_sub
    dom = lax.axis_index("dom")
    sub = lax.axis_index("sub")
    me = dom * n_sub + sub
    tiles, size, feat = features_ref.shape
    rows = tiles * size
    slots = inner_ref.shape[0]
    share = gram_own.shape[0]
    owners = gram_part.shape[0] // share
    mine = lax.div(me * owners + total_devices - 1, total_devices)
    owns = jnp.logical_and(mine < owners, lax.div(mine * total_devices, owners) == me)

    def home(owner):
        return lax.div(owner * total_devices, owners)

    def share_rows(owner):
        return pl.ds(pl.multiple_of(owner * share, share), share)

    incoming = (
        (far_in, far_ref),
        (near_in, near_ref),
        (features_in, features_ref),
        (inner_in, inner_ref),
        (outer_in, outer_ref),
        (dst_in, dst_ref),
        (live_in, live_ref),
        (tile_in, tile_ref),
        (weight_in, weight_ref),
    )
    loads = [
        pltpu.make_async_copy(source, target, load_sems.at[place])
        for place, (source, target) in enumerate(incoming)
    ]

    def device_of(index):
        return (lax.div(index, n_sub), lax.rem(index, n_sub))

    barrier = pltpu.get_barrier_semaphore()

    @pl.loop(1, total_devices)
    def _(offset):
        peer = lax.rem(me + offset, total_devices)
        pl.semaphore_signal(barrier, inc=1, device_id=device_of(peer), device_id_type=MESH)

    for load in loads:
        load.start()
    for load in loads[:3]:
        load.wait()

    features = features_ref[...].reshape(rows, feat)
    far_rows = jnp.dot(
        one_hot_rows(far_ref[...], rows), features, preferred_element_type=jnp.float32
    ).astype(jnp.bfloat16)
    near_rows = jnp.dot(
        one_hot_rows(near_ref[...], rows), features, preferred_element_type=jnp.float32
    ).astype(jnp.bfloat16)
    far_send[...] = far_rows
    near_send[...] = near_rows
    per_dom = far_send.shape[0] // n_dom
    per_sub = near_send.shape[0] // n_sub
    far_count = per_dom * n_dom
    packed = size % per_dom == 0 and size % per_sub == 0 and arrived.shape[0] == table.shape[0] * size

    def place(first, count):
        if packed:
            within = pl.multiple_of(lax.rem(first, size), count)
            return table.at[lax.div(first, size), pl.ds(within, count)]
        return arrived.at[pl.ds(pl.multiple_of(first, count), count)]

    def dom_rows(index):
        return pl.ds(pl.multiple_of(index * per_dom, per_dom), per_dom)

    def sub_rows(index):
        return pl.ds(pl.multiple_of(index * per_sub, per_sub), per_sub)

    def dom_place(index):
        return place(index * per_dom, per_dom)

    def sub_place(index):
        return place(far_count + index * per_sub, per_sub)

    pl.semaphore_wait(barrier, total_devices - 1)

    @pl.loop(1, n_dom)
    def _(offset):
        peer = lax.rem(dom + offset, n_dom)
        pltpu.make_async_remote_copy(
            src_ref=far_send.at[dom_rows(peer)],
            dst_ref=dom_place(dom),
            send_sem=halo_sems.at[0],
            recv_sem=halo_sems.at[1],
            device_id=(peer, sub),
            device_id_type=MESH,
        ).start()

    @pl.loop(1, n_sub)
    def _(offset):
        peer = lax.rem(sub + offset, n_sub)
        pltpu.make_async_remote_copy(
            src_ref=near_send.at[sub_rows(peer)],
            dst_ref=sub_place(sub),
            send_sem=halo_sems.at[2],
            recv_sem=halo_sems.at[3],
            device_id=(dom, peer),
            device_id_type=MESH,
        ).start()

    dom_place(dom)[...] = far_send[dom_rows(dom), :]
    sub_place(sub)[...] = near_send[sub_rows(sub), :]

    def slot_products(rows_ref, source, first):
        for slot in range(slots):
            products[slot] = jnp.dot(
                tile_ref[first + slot],
                rows_ref[source[slot]],
                preferred_element_type=jnp.float32,
            )

    def slot_sum(tile, first, count):
        total = None
        for slot in range(slots):
            target = jnp.full((1, feat), dst_ref[first + slot], jnp.int32)
            chosen = jnp.where(jnp.logical_and(target == tile, count > slot), 1.0, 0.0)
            term = products[slot] * chosen
            total = term if total is None else total + term
        return total

    for load in loads[3:]:
        load.wait()
    slot_products(features_ref, inner_ref, 0)
    inner_count = jnp.full((1, feat), live_ref[0, 0], jnp.int32)
    outer_count = jnp.full((1, feat), live_ref[0, 1], jnp.int32)

    @pl.loop(0, tiles)
    def _(tile):
        acc[tile] = slot_sum(tile, 0, inner_count)

    def settle(ref, sem):
        pltpu.make_async_copy(ref, ref, sem).wait()

    settle(arrived.at[pl.ds(0, per_dom * (n_dom - 1))], halo_sems.at[1])
    settle(arrived.at[pl.ds(0, per_sub * (n_sub - 1))], halo_sems.at[3])
    if not packed:
        table[...] = jnp.dot(
            packing(table.shape[0] * size, arrived.shape[0], n_dom, n_sub, per_dom, per_sub, near_each),
            arrived[...],
            preferred_element_type=jnp.float32,
        ).astype(jnp.bfloat16).reshape(table.shape)
    slot_products(table, outer_ref, slots)

    @pl.loop(0, tiles)
    def _(tile):
        total = acc[tile] + slot_sum(tile, slots, outer_count)
        aggregate[pl.ds(pl.multiple_of(tile * size, size), size), :] = total.astype(jnp.bfloat16)

    projected = jnp.dot(aggregate[...], weight_ref[...], preferred_element_type=jnp.float32)
    hidden = (
        features_ref[...].reshape(rows, feat).astype(jnp.float32) + projected / (1.0 + jnp.exp(-projected))
    ).astype(jnp.bfloat16)
    hidden_t = hidden.T
    blocks = [(top, side) for top in range(0, feat, 128) for side in range(top, feat, 128)]
    for top in range(0, feat, 128):
        stripe = jnp.dot(
            hidden_t[top : top + 128, :], hidden[:, top:], preferred_element_type=jnp.float32
        )
        for side in range(top, feat, 128):
            at = 128 * blocks.index((top, side))
            gram_part[at : at + 128, :] = stripe[:, side - top : side - top + 128]

    @pl.loop(0, owners)
    def _(turn):
        owner = lax.rem(mine + turn, owners)
        peer = home(owner)

        @pl.when(peer != me)
        def _():
            pltpu.make_async_remote_copy(
                src_ref=gram_part.at[share_rows(owner)],
                dst_ref=gram_in.at[me],
                send_sem=sum_sems.at[0],
                recv_sem=sum_sems.at[1],
                device_id=device_of(peer),
                device_id_type=MESH,
            ).start()

    @pl.when(owns)
    def _():
        gram_in[me] = gram_part[share_rows(mine), :]
        settle(gram_in.at[pl.ds(0, total_devices - 1)], sum_sems.at[1])
        total = jnp.sum(gram_in[...], axis=0)
        gram_own[...] = total
        gram[share_rows(mine), :] = total

        @pl.loop(1, total_devices)
        def _(offset):
            peer = lax.rem(me + offset, total_devices)
            pltpu.make_async_remote_copy(
                src_ref=gram_own,
                dst_ref=gram.at[share_rows(mine)],
                send_sem=sum_sems.at[2],
                recv_sem=sum_sems.at[3],
                device_id=device_of(peer),
                device_id_type=MESH,
            ).start()

        settle(gram.at[pl.ds(0, share * (owners - 1))], sum_sems.at[3])

    @pl.when(jnp.logical_not(owns))
    def _():
        settle(gram, sum_sems.at[3])

    vertex_count = rows * total_devices
    diagonal = lax.broadcasted_iota(jnp.int32, (feat, feat), 0) == lax.broadcasted_iota(
        jnp.int32, (feat, feat), 1
    )
    identity = jnp.where(diagonal, 1.0, 0.0)
    for top, side in blocks:
        at = 128 * blocks.index((top, side))
        work[top : top + 128, side : side + 128] = (
            gram[at : at + 128, :] / vertex_count
            + epsilon * identity[top : top + 128, side : side + 128]
        )
        if side > top:
            work[side : side + 128, top : top + 128] = jnp.zeros((128, 128), jnp.float32)
    work[:, feat:] = identity
    for start in range(0, feat, LEAF):
        stop = start + LEAF
        inverse = leaf_inverse(work[start:stop, start:stop])
        pivot_rows = jnp.dot(
            inverse, work[start:stop, :], precision=HIGH, preferred_element_type=jnp.float32
        )
        work[start:stop, :] = pivot_rows
        if stop < feat:
            work[stop:, :] = work[stop:, :] - lax.dot_general(
                pivot_rows[:, stop:feat],
                pivot_rows,
                (((0,), (0,)), ((), ())),
                precision=HIGH,
                preferred_element_type=jnp.float32,
            )

    lower_inverse = work[:, feat:]
    high_part = lower_inverse.astype(jnp.bfloat16)
    low_part = (lower_inverse - high_part.astype(jnp.float32)).astype(jnp.bfloat16)
    across = (((1,), (1,)), ((), ()))
    white = lax.dot_general(
        hidden, high_part, across, preferred_element_type=jnp.float32
    ) + lax.dot_general(hidden, low_part, across, preferred_element_type=jnp.float32)
    result[...] = white.astype(jnp.bfloat16)
    store = pltpu.make_async_copy(result, out_ref, load_sems.at[len(loads)])
    store.start()

    distance = white - features_ref[...].reshape(rows, feat).astype(jnp.float32)
    wide = jnp.sum(distance * distance, axis=0, keepdims=True)
    partial = wide[:, :128]
    for side in range(128, feat, 128):
        partial = partial + wide[:, side : side + 128]
    loss_own[...] = partial
    loss_all[me] = partial

    @pl.loop(1, total_devices)
    def _(offset):
        peer = lax.rem(me + offset, total_devices)
        pltpu.make_async_remote_copy(
            src_ref=loss_own,
            dst_ref=loss_all.at[me],
            send_sem=sum_sems.at[4],
            recv_sem=sum_sems.at[5],
            device_id=device_of(peer),
            device_id_type=MESH,
        ).start()

    settle(far_send.at[pl.ds(0, per_dom * (n_dom - 1))], halo_sems.at[0])
    settle(near_send.at[pl.ds(0, per_sub * (n_sub - 1))], halo_sems.at[2])

    @pl.when(owns)
    def _():
        settle(gram_part.at[pl.ds(0, share * (owners - 1))], sum_sems.at[0])
        settle(gram_in.at[pl.ds(0, total_devices - 1)], sum_sems.at[2])

    @pl.when(jnp.logical_not(owns))
    def _():
        settle(gram_part, sum_sems.at[0])

    settle(loss_all.at[pl.ds(0, total_devices - 1)], sum_sems.at[4])
    settle(loss_all.at[pl.ds(0, total_devices - 1)], sum_sems.at[5])
    loss_ref[0, 0] = jnp.sum(jnp.sum(loss_all[...], axis=0)) / (vertex_count * feat)
    store.wait()


def body(
    n_dom,
    n_sub,
    features,
    weight,
    send_far,
    send_near,
    tile_dst,
    inner_src,
    outer_src,
    tile_live,
    tile_weight,
):
    rows, feat = features.shape
    size = tile_weight.shape[1]
    slots = inner_src.shape[0]
    total = n_dom * n_sub
    tiles_wide = feat // 128
    packed_rows = 128 * (tiles_wide * (tiles_wide + 1) // 2)
    share = 8
    while packed_rows % share or packed_rows // share > total:
        share += 8
    far_count = send_far.shape[0]
    near_count = send_near.shape[0]

    def padded(index, peers):
        each = index.shape[0] // peers
        grid = index.reshape(peers, each)
        return jnp.pad(grid, ((0, 0), (0, padded_rows(each) - each))).reshape(1, -1)

    far_index = padded(send_far, n_dom)
    near_index = padded(send_near, n_sub)
    far_padded = far_index.shape[1]
    near_padded = near_index.shape[1]
    anywhere = pl.BlockSpec(memory_space=pl.ANY)
    smem = pl.BlockSpec(memory_space=pltpu.SMEM)
    f32 = jnp.float32
    bf16 = jnp.bfloat16
    whitened, loss = pl.pallas_call(
        functools.partial(kernel, n_dom, n_sub, near_count // n_sub),
        out_shape=(
            jax.ShapeDtypeStruct((rows, feat), bf16),
            jax.ShapeDtypeStruct((1, 1), f32),
        ),
        in_specs=[anywhere] * 9,
        out_specs=(anywhere, smem),
        scratch_shapes=[
            pltpu.VMEM((rows // size, size, feat), bf16),
            pltpu.VMEM(weight.shape, bf16),
            pltpu.VMEM((1, far_padded), jnp.int32),
            pltpu.VMEM((1, near_padded), jnp.int32),
            pltpu.SMEM(tile_dst.shape, jnp.int32),
            pltpu.SMEM(inner_src.shape, jnp.int32),
            pltpu.SMEM(outer_src.shape, jnp.int32),
            pltpu.SMEM(tile_live.shape, jnp.int32),
            pltpu.VMEM(tile_weight.shape, bf16),
            pltpu.VMEM((rows, feat), bf16),
            pltpu.VMEM((far_padded, feat), bf16),
            pltpu.VMEM((near_padded, feat), bf16),
            pltpu.VMEM((far_padded + near_padded, feat), bf16),
            pltpu.VMEM(((far_count + near_count) // size, size, feat), bf16),
            pltpu.VMEM((slots, size, feat), f32),
            pltpu.VMEM((rows // size, size, feat), f32),
            pltpu.VMEM((rows, feat), bf16),
            pltpu.VMEM((packed_rows, 128), f32),
            pltpu.VMEM((total, share, 128), f32),
            pltpu.VMEM((share, 128), f32),
            pltpu.VMEM((packed_rows, 128), f32),
            pltpu.VMEM((1, 128), f32),
            pltpu.VMEM((total, 1, 128), f32),
            pltpu.VMEM((feat, 2 * feat), f32),
            pltpu.SemaphoreType.DMA((10,)),
            pltpu.SemaphoreType.DMA((4,)),
            pltpu.SemaphoreType.DMA((6,)),
        ],
        compiler_params=pltpu.CompilerParams(collective_id=0, has_side_effects=True),
    )(
        features.reshape(rows // size, size, feat),
        weight,
        far_index,
        near_index,
        tile_dst,
        inner_src,
        outer_src,
        tile_live,
        tile_weight,
    )
    return whitened, loss.reshape(())


def solution(mesh):
    placed = (
        P(("dom", "sub"), None),
        P(),
        P(("dom", "sub")),
        P(("dom", "sub")),
        P(("dom", "sub")),
        P(("dom", "sub")),
        P(("dom", "sub")),
        P(("dom", "sub"), None),
        P(("dom", "sub"), None, None),
    )
    return jax.shard_map(
        functools.partial(body, mesh.shape["dom"], mesh.shape["sub"]),
        mesh=mesh,
        in_specs=placed,
        out_specs=(P(("dom", "sub"), None), P()),
        check_vma=False,
    )
```

```python
import functools

import jax
import jax.numpy as jnp
from jax import lax
from jax.experimental import pallas as pl
from jax.experimental.pallas import tpu as pltpu
from jax.sharding import PartitionSpec as P

epsilon = 1e-05
MESH = pl.DeviceIdType.MESH
LEAF = 64
HIGH = lax.Precision.HIGHEST


def one_hot_rows(index_row, row_count):
    rows = index_row.shape[1]
    columns = jnp.broadcast_to(index_row, (128, rows)).T
    lane = lax.broadcasted_iota(jnp.int32, (rows, 128), 1)
    parts = [
        jnp.where(columns == lane + start, 1.0, 0.0).astype(jnp.bfloat16)
        for start in range(0, row_count, 128)
    ]
    return jnp.concatenate(parts, axis=1)


def padded_rows(count):
    return -(-count // 16) * 16


def packing(packed_rows, padded_total, n_dom, n_sub, per_dom, per_sub, near_rows_each):
    near_total = n_sub * near_rows_each
    far_total = packed_rows - near_total
    far_rows_each = far_total // n_dom
    row = lax.broadcasted_iota(jnp.int32, (packed_rows, padded_total), 0)
    column = lax.broadcasted_iota(jnp.int32, (packed_rows, padded_total), 1)
    far_place = row + lax.div(row, far_rows_each) * (per_dom - far_rows_each)
    near_row = row - far_total
    near_place = (
        n_dom * per_dom + near_row + lax.div(near_row, near_rows_each) * (per_sub - near_rows_each)
    )
    place = jnp.where(row < far_total, far_place, near_place)
    return jnp.where(place == column, 1.0, 0.0).astype(jnp.bfloat16)


def leaf_inverse(block):
    size = block.shape[0]
    row = lax.broadcasted_iota(jnp.int32, (size, size), 0)
    lane = lax.broadcasted_iota(jnp.int32, (size, size), 1)
    work = jnp.concatenate([block, jnp.where(row == lane, 1.0, 0.0)], axis=1)
    group = 8
    done = []
    for step in range(0, size, group):
        lines = [work[i : i + 1, :] for i in range(group)]
        entry = {
            (i, j): jnp.broadcast_to(lines[i][:, step + j : step + j + 1], (1, 2 * size))
            for i in range(group)
            for j in range(i, group)
        }
        inverse = []
        for i in range(group):
            inverse.append(1.0 / entry[i, i])
            for j in range(i + 1, group):
                share = entry[i, j] * inverse[i]
                for k in range(j, group):
                    entry[j, k] = entry[j, k] - share * entry[i, k]
                lines[j] = lines[j] - share * lines[i]
            done.append((lines[i] / jnp.sqrt(entry[i, i]))[:, size:])
        if step + group == size:
            break
        solved = [None] * group
        for i in reversed(range(group)):
            line = lines[i]
            for j in range(i + 1, group):
                line = line - entry[i, j] * solved[j]
            solved[i] = line * inverse[i]
        work = work[group:, :]
        update = work[:, step : step + 1] * solved[0]
        for i in range(1, group):
            update = update + work[:, step + i : step + i + 1] * solved[i]
        work = work - update
    return jnp.concatenate(done, axis=0)


def kernel(
    n_dom,
    n_sub,
    near_each,
    features_in,
    weight_in,
    far_in,
    near_in,
    dst_in,
    inner_in,
    outer_in,
    live_in,
    tile_in,
    out_ref,
    loss_ref,
    features_ref,
    weight_ref,
    far_ref,
    near_ref,
    dst_ref,
    inner_ref,
    outer_ref,
    live_ref,
    tile_ref,
    result,
    far_send,
    near_send,
    arrived,
    table,
    products,
    acc,
    aggregate,
    gram_part,
    gram_in,
    gram_own,
    gram,
    loss_own,
    loss_all,
    work,
    load_sems,
    halo_sems,
    sum_sems,
):
    total_devices = n_dom * n_sub
    dom = lax.axis_index("dom")
    sub = lax.axis_index("sub")
    me = dom * n_sub + sub
    tiles, size, feat = features_ref.shape
    rows = tiles * size
    slots = inner_ref.shape[0]
    share = gram_own.shape[0]
    owners = gram_part.shape[0] // share
    mine = lax.div(me * owners + total_devices - 1, total_devices)
    owns = jnp.logical_and(mine < owners, lax.div(mine * total_devices, owners) == me)

    def home(owner):
        return lax.div(owner * total_devices, owners)

    def share_rows(owner):
        return pl.ds(pl.multiple_of(owner * share, share), share)

    incoming = (
        (far_in, far_ref),
        (near_in, near_ref),
        (features_in, features_ref),
        (inner_in, inner_ref),
        (outer_in, outer_ref),
        (dst_in, dst_ref),
        (live_in, live_ref),
        (tile_in, tile_ref),
        (weight_in, weight_ref),
    )
    loads = [
        pltpu.make_async_copy(source, target, load_sems.at[place])
        for place, (source, target) in enumerate(incoming)
    ]

    def device_of(index):
        return (lax.div(index, n_sub), lax.rem(index, n_sub))

    barrier = pltpu.get_barrier_semaphore()

    @pl.loop(1, total_devices)
    def _(offset):
        peer = lax.rem(me + offset, total_devices)
        pl.semaphore_signal(barrier, inc=1, device_id=device_of(peer), device_id_type=MESH)

    for load in loads:
        load.start()
    for load in loads[:3]:
        load.wait()

    features = features_ref[...].reshape(rows, feat)
    far_rows = jnp.dot(
        one_hot_rows(far_ref[...], rows), features, preferred_element_type=jnp.float32
    ).astype(jnp.bfloat16)
    near_rows = jnp.dot(
        one_hot_rows(near_ref[...], rows), features, preferred_element_type=jnp.float32
    ).astype(jnp.bfloat16)
    far_send[...] = far_rows
    near_send[...] = near_rows
    per_dom = far_send.shape[0] // n_dom
    per_sub = near_send.shape[0] // n_sub
    far_count = per_dom * n_dom
    packed = size % per_dom == 0 and size % per_sub == 0 and arrived.shape[0] == table.shape[0] * size

    def place(first, count):
        if packed:
            within = pl.multiple_of(lax.rem(first, size), count)
            return table.at[lax.div(first, size), pl.ds(within, count)]
        return arrived.at[pl.ds(pl.multiple_of(first, count), count)]

    def dom_rows(index):
        return pl.ds(pl.multiple_of(index * per_dom, per_dom), per_dom)

    def sub_rows(index):
        return pl.ds(pl.multiple_of(index * per_sub, per_sub), per_sub)

    def dom_place(index):
        return place(index * per_dom, per_dom)

    def sub_place(index):
        return place(far_count + index * per_sub, per_sub)

    pl.semaphore_wait(barrier, total_devices - 1)

    @pl.loop(1, n_dom)
    def _(offset):
        peer = lax.rem(dom + offset, n_dom)
        pltpu.make_async_remote_copy(
            src_ref=far_send.at[dom_rows(peer)],
            dst_ref=dom_place(dom),
            send_sem=halo_sems.at[0],
            recv_sem=halo_sems.at[1],
            device_id=(peer, sub),
            device_id_type=MESH,
        ).start()

    @pl.loop(1, n_sub)
    def _(offset):
        peer = lax.rem(sub + offset, n_sub)
        pltpu.make_async_remote_copy(
            src_ref=near_send.at[sub_rows(peer)],
            dst_ref=sub_place(sub),
            send_sem=halo_sems.at[2],
            recv_sem=halo_sems.at[3],
            device_id=(dom, peer),
            device_id_type=MESH,
        ).start()

    dom_place(dom)[...] = far_send[dom_rows(dom), :]
    sub_place(sub)[...] = near_send[sub_rows(sub), :]

    def slot_products(rows_ref, source, first):
        for slot in range(slots):
            products[slot] = jnp.dot(
                tile_ref[first + slot],
                rows_ref[source[slot]],
                preferred_element_type=jnp.float32,
            )

    def slot_sum(tile, first, count):
        total = None
        for slot in range(slots):
            target = jnp.full((1, feat), dst_ref[first + slot], jnp.int32)
            chosen = jnp.where(jnp.logical_and(target == tile, count > slot), 1.0, 0.0)
            term = products[slot] * chosen
            total = term if total is None else total + term
        return total

    for load in loads[3:]:
        load.wait()
    slot_products(features_ref, inner_ref, 0)
    inner_count = jnp.full((1, feat), live_ref[0, 0], jnp.int32)
    outer_count = jnp.full((1, feat), live_ref[0, 1], jnp.int32)

    @pl.loop(0, tiles)
    def _(tile):
        acc[tile] = slot_sum(tile, 0, inner_count)

    def settle(ref, sem):
        pltpu.make_async_copy(ref, ref, sem).wait()

    settle(arrived.at[pl.ds(0, per_dom * (n_dom - 1))], halo_sems.at[1])
    settle(arrived.at[pl.ds(0, per_sub * (n_sub - 1))], halo_sems.at[3])
    if not packed:
        table[...] = jnp.dot(
            packing(table.shape[0] * size, arrived.shape[0], n_dom, n_sub, per_dom, per_sub, near_each),
            arrived[...],
            preferred_element_type=jnp.float32,
        ).astype(jnp.bfloat16).reshape(table.shape)
    slot_products(table, outer_ref, slots)

    @pl.loop(0, tiles)
    def _(tile):
        total = acc[tile] + slot_sum(tile, slots, outer_count)
        aggregate[pl.ds(pl.multiple_of(tile * size, size), size), :] = total.astype(jnp.bfloat16)

    projected = jnp.dot(aggregate[...], weight_ref[...], preferred_element_type=jnp.float32)
    hidden = (
        features_ref[...].reshape(rows, feat).astype(jnp.float32) + projected / (1.0 + jnp.exp(-projected))
    ).astype(jnp.bfloat16)
    hidden_t = hidden.T
    blocks = [(top, side) for top in range(0, feat, 128) for side in range(top, feat, 128)]
    for top in range(0, feat, 128):
        stripe = jnp.dot(
            hidden_t[top : top + 128, :], hidden[:, top:], preferred_element_type=jnp.float32
        )
        for side in range(top, feat, 128):
            at = 128 * blocks.index((top, side))
            gram_part[at : at + 128, :] = stripe[:, side - top : side - top + 128]

    @pl.loop(0, owners)
    def _(turn):
        owner = lax.rem(mine + turn, owners)
        peer = home(owner)

        @pl.when(peer != me)
        def _():
            pltpu.make_async_remote_copy(
                src_ref=gram_part.at[share_rows(owner)],
                dst_ref=gram_in.at[me],
                send_sem=sum_sems.at[0],
                recv_sem=sum_sems.at[1],
                device_id=device_of(peer),
                device_id_type=MESH,
            ).start()

    @pl.when(owns)
    def _():
        gram_in[me] = gram_part[share_rows(mine), :]
        settle(gram_in.at[pl.ds(0, total_devices - 1)], sum_sems.at[1])
        total = jnp.sum(gram_in[...], axis=0)
        gram_own[...] = total
        gram[share_rows(mine), :] = total

        @pl.loop(1, total_devices)
        def _(offset):
            peer = lax.rem(me + offset, total_devices)
            pltpu.make_async_remote_copy(
                src_ref=gram_own,
                dst_ref=gram.at[share_rows(mine)],
                send_sem=sum_sems.at[2],
                recv_sem=sum_sems.at[3],
                device_id=device_of(peer),
                device_id_type=MESH,
            ).start()

        settle(gram.at[pl.ds(0, share * (owners - 1))], sum_sems.at[3])

    @pl.when(jnp.logical_not(owns))
    def _():
        settle(gram, sum_sems.at[3])

    vertex_count = rows * total_devices
    diagonal = lax.broadcasted_iota(jnp.int32, (feat, feat), 0) == lax.broadcasted_iota(
        jnp.int32, (feat, feat), 1
    )
    identity = jnp.where(diagonal, 1.0, 0.0)
    for top, side in blocks:
        at = 128 * blocks.index((top, side))
        work[top : top + 128, side : side + 128] = (
            gram[at : at + 128, :] / vertex_count
            + epsilon * identity[top : top + 128, side : side + 128]
        )
        if side > top:
            work[side : side + 128, top : top + 128] = jnp.zeros((128, 128), jnp.float32)
    work[:, feat:] = identity
    for start in range(0, feat, LEAF):
        stop = start + LEAF
        inverse = leaf_inverse(work[start:stop, start:stop])
        pivot_rows = jnp.dot(
            inverse, work[start:stop, :], precision=HIGH, preferred_element_type=jnp.float32
        )
        work[start:stop, :] = pivot_rows
        if stop < feat:
            work[stop:, :] = work[stop:, :] - lax.dot_general(
                pivot_rows[:, stop:feat],
                pivot_rows,
                (((0,), (0,)), ((), ())),
                precision=HIGH,
                preferred_element_type=jnp.float32,
            )

    lower_inverse = work[:, feat:]
    high_part = lower_inverse.astype(jnp.bfloat16)
    low_part = (lower_inverse - high_part.astype(jnp.float32)).astype(jnp.bfloat16)
    across = (((1,), (1,)), ((), ()))
    white = lax.dot_general(
        hidden, high_part, across, preferred_element_type=jnp.float32
    ) + lax.dot_general(hidden, low_part, across, preferred_element_type=jnp.float32)
    result[...] = white.astype(jnp.bfloat16)
    store = pltpu.make_async_copy(result, out_ref, load_sems.at[len(loads)])
    store.start()

    distance = white - features_ref[...].reshape(rows, feat).astype(jnp.float32)
    wide = jnp.sum(distance * distance, axis=0, keepdims=True)
    partial = wide[:, :128]
    for side in range(128, feat, 128):
        partial = partial + wide[:, side : side + 128]
    loss_own[...] = partial
    loss_all[me] = partial

    @pl.loop(1, total_devices)
    def _(offset):
        peer = lax.rem(me + offset, total_devices)
        pltpu.make_async_remote_copy(
            src_ref=loss_own,
            dst_ref=loss_all.at[me],
            send_sem=sum_sems.at[4],
            recv_sem=sum_sems.at[5],
            device_id=device_of(peer),
            device_id_type=MESH,
        ).start()

    settle(far_send.at[pl.ds(0, per_dom * (n_dom - 1))], halo_sems.at[0])
    settle(near_send.at[pl.ds(0, per_sub * (n_sub - 1))], halo_sems.at[2])

    @pl.when(owns)
    def _():
        settle(gram_part.at[pl.ds(0, share * (owners - 1))], sum_sems.at[0])
        settle(gram_in.at[pl.ds(0, total_devices - 1)], sum_sems.at[2])

    @pl.when(jnp.logical_not(owns))
    def _():
        settle(gram_part, sum_sems.at[0])

    settle(loss_all.at[pl.ds(0, total_devices - 1)], sum_sems.at[4])
    settle(loss_all.at[pl.ds(0, total_devices - 1)], sum_sems.at[5])
    loss_ref[0, 0] = jnp.sum(jnp.sum(loss_all[...], axis=0)) / (vertex_count * feat)
    store.wait()


def body(
    n_dom,
    n_sub,
    features,
    weight,
    send_far,
    send_near,
    tile_dst,
    inner_src,
    outer_src,
    tile_live,
    tile_weight,
):
    rows, feat = features.shape
    size = tile_weight.shape[1]
    slots = inner_src.shape[0]
    total = n_dom * n_sub
    tiles_wide = feat // 128
    packed_rows = 128 * (tiles_wide * (tiles_wide + 1) // 2)
    share = 8
    while packed_rows % share or packed_rows // share > total:
        share += 8
    far_count = send_far.shape[0]
    near_count = send_near.shape[0]

    def padded(index, peers):
        each = index.shape[0] // peers
        grid = index.reshape(peers, each)
        return jnp.pad(grid, ((0, 0), (0, padded_rows(each) - each))).reshape(1, -1)

    far_index = padded(send_far, n_dom)
    near_index = padded(send_near, n_sub)
    far_padded = far_index.shape[1]
    near_padded = near_index.shape[1]
    anywhere = pl.BlockSpec(memory_space=pl.ANY)
    smem = pl.BlockSpec(memory_space=pltpu.SMEM)
    f32 = jnp.float32
    bf16 = jnp.bfloat16
    whitened, loss = pl.pallas_call(
        functools.partial(kernel, n_dom, n_sub, near_count // n_sub),
        out_shape=(
            jax.ShapeDtypeStruct((rows, feat), bf16),
            jax.ShapeDtypeStruct((1, 1), f32),
        ),
        in_specs=[anywhere] * 9,
        out_specs=(anywhere, smem),
        scratch_shapes=[
            pltpu.VMEM((rows // size, size, feat), bf16),
            pltpu.VMEM(weight.shape, bf16),
            pltpu.VMEM((1, far_padded), jnp.int32),
            pltpu.VMEM((1, near_padded), jnp.int32),
            pltpu.SMEM(tile_dst.shape, jnp.int32),
            pltpu.SMEM(inner_src.shape, jnp.int32),
            pltpu.SMEM(outer_src.shape, jnp.int32),
            pltpu.SMEM(tile_live.shape, jnp.int32),
            pltpu.VMEM(tile_weight.shape, bf16),
            pltpu.VMEM((rows, feat), bf16),
            pltpu.VMEM((far_padded, feat), bf16),
            pltpu.VMEM((near_padded, feat), bf16),
            pltpu.VMEM((far_padded + near_padded, feat), bf16),
            pltpu.VMEM(((far_count + near_count) // size, size, feat), bf16),
            pltpu.VMEM((slots, size, feat), f32),
            pltpu.VMEM((rows // size, size, feat), f32),
            pltpu.VMEM((rows, feat), bf16),
            pltpu.VMEM((packed_rows, 128), f32),
            pltpu.VMEM((total, share, 128), f32),
            pltpu.VMEM((share, 128), f32),
            pltpu.VMEM((packed_rows, 128), f32),
            pltpu.VMEM((1, 128), f32),
            pltpu.VMEM((total, 1, 128), f32),
            pltpu.VMEM((feat, 2 * feat), f32),
            pltpu.SemaphoreType.DMA((10,)),
            pltpu.SemaphoreType.DMA((4,)),
            pltpu.SemaphoreType.DMA((6,)),
        ],
        compiler_params=pltpu.CompilerParams(collective_id=0, has_side_effects=True),
    )(
        features.reshape(rows // size, size, feat),
        weight,
        far_index,
        near_index,
        tile_dst,
        inner_src,
        outer_src,
        tile_live,
        tile_weight,
    )
    return whitened, loss.reshape(())


def solution(mesh):
    placed = (
        P(("dom", "sub"), None),
        P(),
        P(("dom", "sub")),
        P(("dom", "sub")),
        P(("dom", "sub")),
        P(("dom", "sub")),
        P(("dom", "sub")),
        P(("dom", "sub"), None),
        P(("dom", "sub"), None, None),
    )
    return jax.shard_map(
        functools.partial(body, mesh.shape["dom"], mesh.shape["sub"]),
        mesh=mesh,
        in_specs=placed,
        out_specs=(P(("dom", "sub"), None), P()),
        check_vma=False,
    )
```
